32 devices in a mesh: dp: 8 (over z, y), mp: 4 (over x, core).
Axes of the slice: x: 2, y: 2, z: 4, core: 2. Of those that a mesh axis runs over, the one named last changes fastest.
Arguments:
- queries: bfloat16 [4096, 4096], P('dp', 'mp'), may hold values from -150 to 150, as said below
- keys: bfloat16 [4096, 4096], P('dp', 'mp'), may hold values from -8 to 8
- values: bfloat16 [4096, 4096], P('dp', 'mp'), may hold values from -6 to 6
- out_weight: bfloat16 [4096, 2048], P('mp', 'dp'), may hold values from -0.125 to 0.125
- span_start: int32 [8], P('dp'), may hold values from 1 to 3
- span_len: int32 [8], P('dp'), may hold values from 1 to 3
Outputs:
- projected: bfloat16 [4096, 2048], P('dp', 'mp')
The draws below stay inside these ranges and needn't reach their ends.
Inputs may be any that keep to these rules, and one draw needn't show every extreme that they name: `queries`: without the hidden law's aligned rows, entries are standard normal values clipped to 8 in magnitude.
All inputs are finite; a program needn't handle non-finite values.
Results may differ from the reference program's by a relative error of at most 0.0068.
Values may be sent and summed in bfloat16 or wider, within the bound.
No kernel may reach another device: no remote copies, remote signals or barrier semaphores. Data moves between devices by JAX's collectives and lax.ppermute only.
A program may use at most 64 MiB of HBM per device.

```python
import jax
import jax.numpy as jnp
from jax import lax

HEADS = 32
HD = 128
D = 4096
OUT_WIN = 2048
SEQ = 512
BLK = 128
NB = 4
TOKENS = 4096
N_DP = 8


def paired_rows(key):
    key_rows = jnp.clip(jax.random.normal(jax.random.fold_in(key, 12), (TOKENS, D), jnp.float32), -8.0, 8.0)
    query_rows = jnp.clip(jax.random.normal(jax.random.fold_in(key, 11), (TOKENS, D), jnp.float32), -8.0, 8.0)
    return (query_rows, key_rows)


def draw_queries(key, part):
    return paired_rows(key)[0].astype(jnp.bfloat16)


def draw_keys(key, part):
    return paired_rows(key)[1].astype(jnp.bfloat16)


def plant(values, own_key, low, largest):
    extent = values.shape
    index_at = [jax.random.randint(jax.random.fold_in(own_key, axis), (), 0, extent[axis]) for axis in range(len(extent))]
    values = values.at[tuple(index_at)].set(low)
    longest = extent.index(max(extent))
    index_at[longest] = (index_at[longest] + 1) % extent[longest]
    return values.at[tuple(index_at)].set(largest)


def with_spikes(array, stream_key, source, target, parts, factor):
    def block_of(axis_at):
        return (jnp.arange(array.shape[axis_at]) // (array.shape[axis_at] // parts)).reshape((-1,) + (1,) * (array.ndim - 1 - axis_at))

    near = jax.random.permutation(stream_key, parts)[block_of(target)]
    other_side = (block_of(target) + parts // 2) % parts
    return jnp.where((block_of(source) == near) | (block_of(source) == other_side), factor * array, array)


def level_of(key, extent, pieces, smallest, largest):
    def one(dim, parts):
        draws = jax.random.uniform(jax.random.fold_in(jax.random.fold_in(key, 6), dim), (parts,), jnp.float32, smallest / len(pieces), largest / len(pieces))
        return jnp.repeat(jnp.exp(draws), extent[dim] // parts).reshape((-1,) + (1,) * (len(extent) - dim - 1))

    loudness = one(*pieces[0])
    for cut in pieces[1:]:
        loudness = loudness * one(*cut)
    return loudness


def scatter_about(own_key, shape, spread, limit, shards=(), kind=jnp.bfloat16):
    drawn = spread * jax.random.normal(own_key, shape, jnp.float32)
    if shards:
        drawn = drawn * level_of(own_key, shape, shards, -0.22, 0.18)
    return jnp.clip(drawn, -limit, limit).astype(kind)


def gaussian_with(stream_key, dims, width, most, shards, heavy, kind=jnp.bfloat16):
    values = width * jax.random.normal(stream_key, dims, jnp.float32)
    if shards:
        values = values * level_of(stream_key, dims, shards, -0.22, 0.18)
    return jnp.clip(with_spikes(values, jax.random.fold_in(stream_key, 3), *heavy), -most, most).astype(kind)


def setup_inputs(seed: int = 0) -> dict:
    seeds = jax.random.split(jax.random.key(seed), 7)
    return {
        "queries": draw_queries(jax.random.fold_in(seeds[6], 71), 0),
        "keys": draw_keys(jax.random.fold_in(seeds[6], 71), 0),
        "values": scatter_about(seeds[2], (TOKENS, D), 1.0, 6.0, ((0, 8), (1, 4))),
        "out_weight": gaussian_with(seeds[3], (D, OUT_WIN), D ** -0.5, 0.125, ((0, 4), (1, 8)), (0, 1, 8, 2.0)),
        "span_start": plant(jax.random.randint(seeds[4], (N_DP,), 1, NB), jax.random.fold_in(seeds[4], 1), 1, NB - 1).astype(jnp.int32),
        "span_len": plant(jax.random.randint(seeds[5], (N_DP,), 1, NB), jax.random.fold_in(seeds[5], 1), 1, NB - 1).astype(jnp.int32),
    }


def attend_one(query_rows, key_rows, value_rows, start, length):
    position = jnp.arange(SEQ, dtype=jnp.int32)
    block = position // BLK
    finish = jnp.minimum(start + length, NB)
    image = (block >= start) & (block < finish)
    causal = position[None, :] <= position[:, None]
    allowed = jnp.where(image[:, None], image[None, :], causal)
    query_f = query_rows.reshape(SEQ, HEADS, HD).astype(jnp.float32)
    key_f = key_rows.reshape(SEQ, HEADS, HD).astype(jnp.float32)
    value_f = value_rows.reshape(SEQ, HEADS, HD).astype(jnp.float32)
    scores = jnp.einsum('qhd,khd->hqk', query_f, key_f) / jnp.sqrt(jnp.float32(HD))
    scores = jnp.where(allowed[None, :, :], scores, jnp.float32(-1e+30))
    top = lax.optimization_barrier(jnp.max(scores, axis=-1, keepdims=True))
    expo = jnp.exp(scores - top)
    weights = (expo / lax.optimization_barrier(jnp.sum(expo, axis=-1, keepdims=True))).astype(jnp.bfloat16)
    result = jnp.einsum('hqk,khd->qhd', weights.astype(jnp.float32), value_f)
    return result.astype(jnp.bfloat16).reshape(SEQ, D)

def reference(queries, keys, values, out_weight, span_start, span_len):

    def one(items):
        return attend_one(items[0], items[1], items[2], items[3], items[4])
    attended = lax.map(one, (queries.reshape(N_DP, SEQ, D), keys.reshape(N_DP, SEQ, D), values.reshape(N_DP, SEQ, D), span_start.astype(jnp.int32), span_len.astype(jnp.int32)))
    attended = attended.reshape(TOKENS, D)
    return jnp.dot(attended, out_weight, preferred_element_type=jnp.float32).astype(jnp.bfloat16)
```

```python
import jax
import jax.numpy as jnp
import numpy as np
from jax import lax
from jax.sharding import PartitionSpec as P

HD = 128
BLK = 128


def attend_local(query_rows, key_rows, value_rows, start, length):
    rows = query_rows.shape[0]
    heads_here = query_rows.shape[1] // HD
    position = jnp.arange(rows, dtype=jnp.int32)
    block = position // BLK
    finish = jnp.minimum(start + length, rows // BLK)
    image = (block >= start) & (block < finish)
    causal = position[None, :] <= position[:, None]
    allowed = jnp.where(image[:, None], image[None, :], causal)
    query_h = query_rows.reshape(rows, heads_here, HD)
    key_h = key_rows.reshape(rows, heads_here, HD)
    value_h = value_rows.reshape(rows, heads_here, HD)
    scores = jnp.einsum("qhd,khd->hqk", query_h, key_h, preferred_element_type=jnp.float32)
    scores = scores / jnp.sqrt(jnp.float32(HD))
    scores = jnp.where(allowed[None, :, :], scores, jnp.float32(-1e30))
    top = jnp.max(scores, axis=-1, keepdims=True)
    expo = jnp.exp(scores - top)
    weights = (expo / jnp.sum(expo, axis=-1, keepdims=True)).astype(jnp.bfloat16)
    result = jnp.einsum("hqk,khd->qhd", weights, value_h, preferred_element_type=jnp.float32)
    return result.astype(jnp.bfloat16).reshape(rows, heads_here * HD)


def shards_gathered(queries, keys, values, out_weight, span_start, span_len):
    attended = attend_local(queries, keys, values, span_start[0], span_len[0])
    whole = lax.all_gather(out_weight, "dp", axis=1, tiled=True)
    partial_sums = jnp.dot(attended, whole, preferred_element_type=jnp.float32)
    summed = lax.psum_scatter(partial_sums, "mp", scatter_dimension=1, tiled=True)
    return summed.astype(jnp.bfloat16)


def make_ring(n_dp, n_mp):
    order = list(range(0, n_dp, 2)) + list(range(n_dp - 1, 0, -2))
    spot_of = [order.index(d) for d in range(n_dp)]
    ahead = [(order[i], order[(i + 1) % n_dp]) for i in range(n_dp)]
    back = [(b, a) for a, b in ahead]
    half = n_dp // 2
    per_owner = n_dp // n_mp

    def owner(spot):
        return order[spot % n_dp] // per_owner

    firsts = (-2, -1, 1, 0) if half == 4 else tuple(range(-half + 1, 1))
    table = np.zeros((n_dp * n_mp, 2 * len(firsts)), np.int32)
    for d in range(n_dp):
        for m in range(n_mp):
            for k, first in enumerate(firsts):
                one, two = order[(spot_of[d] + first) % n_dp], order[(spot_of[d] + first + half) % n_dp]
                keeps_one = (one // per_owner) % 2 == m % 2
                kept = one if keeps_one else two
                table[d * n_mp + m, 2 * k] = keeps_one
                table[d * n_mp + m, 2 * k + 1] = kept % per_owner if kept // per_owner == m else -1

    def shards(queries, keys, values, out_weight, span_start, span_len):
        rows, width = out_weight.shape
        dp, mp = lax.axis_index("dp"), lax.axis_index("mp")
        facts = jnp.asarray(table)[dp * n_mp + mp]
        ups = {"a": {0: out_weight[: rows // 2]}, "b": {0: out_weight[rows // 2 :]}}
        downs = {"a": {0: ups["a"][0]}, "b": {0: ups["b"][0]}}
        for step in range(1, half + 1):
            ups["a"][step] = lax.ppermute(ups["a"][step - 1], "dp", ahead)
            downs["b"][step] = lax.ppermute(downs["b"][step - 1], "dp", back)
            if step < half:
                ups["b"][step] = lax.ppermute(ups["b"][step - 1], "dp", ahead)
                downs["a"][step] = lax.ppermute(downs["a"][step - 1], "dp", back)
        attended = attend_local(queries, keys, values, span_start[0], span_len[0])
        left, right = attended[:, : rows // 2], attended[:, rows // 2 :]

        def product(offset):
            if offset == half:
                upper, lower = ups["a"][half], downs["b"][half]
            elif offset <= 0:
                upper, lower = ups["a"][-offset], ups["b"][-offset]
            else:
                upper, lower = downs["a"][offset], downs["b"][offset]
            return jnp.dot(left, upper, preferred_element_type=jnp.float32) + jnp.dot(
                right, lower, preferred_element_type=jnp.float32
            )

        pieces = []
        for k, first in enumerate(firsts):
            second = first + half if first <= 0 else first - half
            one, two = product(first), product(second)
            mine = facts[2 * k] == 1
            keep = jnp.where(mine, one, two)
            send = jnp.where(mine, two, one).astype(jnp.bfloat16)
            got = lax.ppermute(send, "mp", [(m, m ^ 1) for m in range(n_mp)])
            keep = keep + got.astype(jnp.float32)
            across = []
            for place in range(n_dp):
                for offset in (first, second):
                    to = owner(place + offset)
                    across.append((order[place] * n_mp + (to ^ 2), order[place] * n_mp + to))
            got = lax.ppermute(keep.astype(jnp.bfloat16), ("dp", "mp"), across)
            pieces.append((facts[2 * k + 1], keep + got.astype(jnp.float32)))
        columns = []
        for at in range(per_owner):
            total = jnp.zeros(pieces[0][1].shape, jnp.float32)
            for slot, value in pieces:
                total = jnp.where(slot == at, value, total)
            columns.append(total.astype(jnp.bfloat16))
        return jnp.concatenate(columns, axis=1)

    return shards


def solution(mesh):
    in_specs = (P("dp", "mp"), P("dp", "mp"), P("dp", "mp"), P("mp", "dp"), P("dp"), P("dp"))
    out_specs = P("dp", "mp")
    n_dp, n_mp = mesh.shape["dp"], mesh.shape["mp"]
    if n_mp == 4 and n_dp % 8 == 0 and n_dp <= 16:
        shards = make_ring(n_dp, n_mp)
    else:
        shards = shards_gathered
    return jax.shard_map(shards, mesh=mesh, in_specs=in_specs, out_specs=out_specs, check_vma=False)
```

```python
import functools

import jax
import jax.numpy as jnp
from jax import lax
from jax.experimental import pallas as pl
from jax.experimental.pallas import tpu as pltpu
from jax.sharding import PartitionSpec as P

HD = 128
BLK = 128


def attention_kernel(start_ref, length_ref, query_ref, key_ref, value_ref, out_ref, bias_ref):
    rows = query_ref.shape[0]

    @pl.when(pl.program_id(0) == 0)
    def _():
        finish = jnp.minimum(start_ref[0] + length_ref[0], rows // BLK)
        q_at = lax.broadcasted_iota(jnp.int32, (rows, rows), 0)
        k_at = lax.broadcasted_iota(jnp.int32, (rows, rows), 1)
        low, high = start_ref[0] * BLK, finish * BLK
        q_image = (q_at >= low) & (q_at < high)
        k_image = (k_at >= low) & (k_at < high)
        allowed = (q_image & k_image) | (jnp.logical_not(q_image) & (k_at <= q_at))
        bias_ref[...] = jnp.where(allowed, 0.0, -1e30)

    for at in range(0, query_ref.shape[1], HD):
        head = slice(at, at + HD)
        scores = lax.dot_general(
            query_ref[:, head], key_ref[:, head], (((1,), (1,)), ((), ())), preferred_element_type=jnp.float32
        )
        scores = scores + bias_ref[...]
        top = jnp.max(scores, axis=-1, keepdims=True)
        expo = jnp.exp2((scores - top) * (1.4426950408889634 / HD**0.5))
        weights = (expo * (1.0 / jnp.sum(expo, axis=-1, keepdims=True))).astype(jnp.bfloat16)
        result = jnp.dot(weights, value_ref[:, head], preferred_element_type=jnp.float32)
        out_ref[:, head] = result.astype(jnp.bfloat16)


def attend_local(query_rows, key_rows, value_rows, start, length):
    rows, width = query_rows.shape
    heads = width // HD
    wide = 4 * HD if heads % 4 == 0 else HD
    block = pl.BlockSpec((rows, wide), lambda h: (0, h))
    return pl.pallas_call(
        attention_kernel,
        grid=(width // wide,),
        in_specs=[pl.BlockSpec(memory_space=pltpu.SMEM)] * 2 + [block] * 3,
        out_specs=block,
        out_shape=jax.ShapeDtypeStruct((rows, width), jnp.bfloat16),
        scratch_shapes=[pltpu.VMEM((rows, rows), jnp.float32)],
        compiler_params=pltpu.CompilerParams(dimension_semantics=("arbitrary",), vmem_limit_bytes=60 * 2**20),
        cost_estimate=pl.CostEstimate(
            flops=16 * rows * rows * width, bytes_accessed=8 * rows * width, transcendentals=heads * rows * rows
        ),
    )(start, length, query_rows, key_rows, value_rows)


def shards_gathered(queries, keys, values, out_weight, span_start, span_len):
    attended = attend_local(queries, keys, values, span_start, span_len)
    whole = lax.all_gather(out_weight, "dp", axis=1, tiled=True)
    partial_sums = jnp.dot(attended, whole, preferred_element_type=jnp.float32)
    summed = lax.psum_scatter(partial_sums, "mp", scatter_dimension=1, tiled=True)
    return summed.astype(jnp.bfloat16)


def make_ring(n_dp, n_mp):
    order = list(range(0, n_dp, 2)) + list(range(n_dp - 1, 0, -2))
    spot_of = [order.index(d) for d in range(n_dp)]
    ahead = [(order[i], order[(i + 1) % n_dp]) for i in range(n_dp)]
    back = [(b, a) for a, b in ahead]
    half = n_dp // 2
    per_owner = n_dp // n_mp

    def owner(spot):
        return order[spot % n_dp] // per_owner

    firsts = sorted(range(-half + 1, 1), key=lambda f: max(abs(f), half - abs(f)))
    def facts(offset):
        dp, mp = lax.axis_index("dp"), lax.axis_index("mp")
        spot = jnp.where(dp % 2 == 0, dp // 2, n_dp - 1 - dp // 2)

        def block(at):
            at = lax.rem(spot + at + n_dp, n_dp)
            return jnp.where(at < half, 2 * at, 2 * (n_dp - 1 - at) + 1)

        one, two = block(offset), block(offset + half)
        keeps = (one // per_owner) % 2 == mp % 2
        kept = jnp.where(keeps, one, two)
        return keeps, jnp.where(kept // per_owner == mp, kept % per_owner, -1)

    def unit_kernel(offset, attended, upper_1, lower_1, upper_2, lower_2, keep, send):
        mid = attended.shape[1] // 2
        left, right = attended[:, :mid], attended[:, mid:]
        keeps, _ = facts(offset)
        one = jnp.dot(left, upper_1[...], preferred_element_type=jnp.float32)
        one += jnp.dot(right, lower_1[...], preferred_element_type=jnp.float32)
        two = jnp.dot(left, upper_2[...], preferred_element_type=jnp.float32)
        two += jnp.dot(right, lower_2[...], preferred_element_type=jnp.float32)
        keep[...] = jnp.where(keeps, one, two)
        send[...] = jnp.where(keeps, two, one).astype(jnp.bfloat16)

    def place_kernel(offsets, *refs):
        out = refs[-1]
        if len(refs) % 2 == 0:
            out[...] = refs[-2][...]
        for k, offset in enumerate(offsets):
            _, slot = facts(offset)
            for at in range(per_owner):

                @pl.when(slot == at)
                def _():
                    mine, got = refs[2 * k], refs[2 * k + 1]
                    width = mine.shape[1]
                    out[:, at * width : (at + 1) * width] = (mine[...] + got[...].astype(jnp.float32)).astype(
                        jnp.bfloat16
                    )

    def call(name, kernel, out_shape, flops, *operands):
        size = sum(x.size * x.dtype.itemsize for x in operands)
        with jax.named_scope(name):
            return pl.pallas_call(
                kernel,
                out_shape=out_shape,
                compiler_params=pltpu.CompilerParams(vmem_limit_bytes=24 * 2**20),
                cost_estimate=pl.CostEstimate(flops=flops, bytes_accessed=size, transcendentals=0),
            )(*operands)

    def hop(name, value, pairs, axis="dp"):
        with jax.named_scope(name):
            return lax.ppermute(value, axis, pairs)

    def shards(queries, keys, values, out_weight, span_start, span_len):
        rows, width = out_weight.shape
        mid = rows // 2
        with jax.named_scope("attend"):
            attended = attend_local(queries, keys, values, span_start, span_len)
        tokens = attended.shape[0]
        up = hop("u1", out_weight, ahead)
        down = hop("d1", out_weight, back)
        blocks = {0: (out_weight[:mid], out_weight[mid:]), -1: (up[:mid], up[mid:]), 1: (down[:mid], down[mid:])}
        for step in range(2, half + 1):
            ua = hop(f"u{step}a", blocks[1 - step][0], ahead)
            db = hop(f"d{step}b", blocks[step - 1][1], back)
            if step < half:
                ub = hop(f"u{step}b", blocks[1 - step][1], ahead)
                da = hop(f"d{step}a", blocks[step - 1][0], back)
                blocks[-step], blocks[step] = (ua, ub), (da, db)
            else:
                blocks[half] = (ua, db)

        pieces, out = [], ()
        for k, first in enumerate(firsts):
            shapes = [jax.ShapeDtypeStruct((tokens, width), t) for t in (jnp.float32, jnp.bfloat16)]
            keep, send = call(
                f"unit{k}",
                functools.partial(unit_kernel, first),
                shapes,
                32 * tokens * rows * width,
                attended,
                *blocks[first],
                *blocks[first + half],
            )
            got = hop(f"c{k}", send, [(m, m ^ 1) for m in range(n_mp)], "mp")
            keep = keep + got.astype(jnp.float32)
            across = []
            for place in range(n_dp):
                for offset in (first, first + half):
                    to = owner(place + offset)
                    across.append((order[place] * n_mp + (to ^ 2), order[place] * n_mp + to))
            got = hop(f"x{k}", keep.astype(jnp.bfloat16), across, ("dp", "mp"))
            pieces += [keep, got]
            if k >= len(firsts) - 2:
                last = k == len(firsts) - 1
                out = (
                    call(
                        f"place{k}",
                        functools.partial(place_kernel, [first] if last else firsts[:-1]),
                        jax.ShapeDtypeStruct((tokens, width * per_owner), jnp.bfloat16),
                        tokens * width,
                        *pieces,
                        *out,
                    ),
                )
                pieces = []
        return out[0]

    return shards


def solution(mesh):
    in_specs = (P("dp", "mp"), P("dp", "mp"), P("dp", "mp"), P("mp", "dp"), P("dp"), P("dp"))
    out_specs = P("dp", "mp")
    n_dp, n_mp = mesh.shape["dp"], mesh.shape["mp"]
    if n_mp == 4 and n_dp % 8 == 0 and n_dp <= 16:
        shards = make_ring(n_dp, n_mp)
    else:
        shards = shards_gathered
    return jax.shard_map(shards, mesh=mesh, in_specs=in_specs, out_specs=out_specs, check_vma=False)
```
